256 devices in a mesh: fsdp: 16 (over y, x), rep: 16 (over z, core).
Axes of the slice: x: 4, y: 4, z: 8, core: 2. Of those that a mesh axis runs over, the one named last changes fastest.
Arguments:
- gradient: float32 [11264, 8192], P('fsdp', 'rep'), may hold values from -6 to 6
- row_counts: int32 [16], replicated, may hold values from 1 to 704, 8192 in all
- owners: int32 [16, 16], P(None, 'rep'), may hold values from 0 to 15, as said below
- refresh_flags: int32 [16, 16], P(None, 'rep'), may hold values 0 or 1
- stat_left: float32 [16, 16, 512, 512], P('fsdp', 'rep'), as said below
- stat_right: float32 [16, 16, 512, 512], P('fsdp', 'rep'), as said below
- root_left: float32 [16, 16, 512, 512], P('fsdp', 'rep'), as said below
- root_right: float32 [16, 16, 512, 512], P('fsdp', 'rep'), as said below
Outputs:
- direction: bfloat16 [11264, 8192], P('fsdp')
- new_left: float32 [16, 16, 512, 512], P('fsdp', 'rep')
- new_right: float32 [16, 16, 512, 512], P('fsdp', 'rep')
The draws below stay inside these ranges and needn't reach their ends.
Inputs may be any that keep to these rules, and one draw needn't show every extreme that they name: `owners`: in each column band of blocks every fsdp index owns exactly 1 block. `stat_left`: symmetric positive definite. `stat_right`: symmetric positive definite. `root_left`: symmetric positive definite. `root_right`: symmetric positive definite.
All inputs are finite; a program needn't handle non-finite values. No bound on the sum of `refresh_flags` on one device may be relied on, other than what follows from the above.
Results may differ from the reference program's by a relative error of at most 0.001.
Values may be sent and summed in bfloat16 or wider, within the bound.
No kernel may reach another device: no remote copies, remote signals or barrier semaphores. Data moves between devices by JAX's collectives and lax.ppermute only.
A program may use at most 128 MiB of HBM per device.

```python
import math
import jax
import jax.numpy as jnp
import numpy as np
from jax import lax

COLS = 8192
ROWS = 8192
BLOCK = 512
ITERS = 3
CAP = 704
BANDS = 16
NCB = 16
SLOTS = 1
N_FSDP = 16


def definite(key, low, high):
    shape = (N_FSDP * SLOTS, NCB, BLOCK, BLOCK)
    offdiag = 0.8 / jnp.sqrt(float(BLOCK))
    uniform_noise = jax.random.uniform(jax.random.fold_in(key, 1), shape, jnp.float32, -1.0, 1.0)
    symmetric = 0.5 * (uniform_noise + jnp.swapaxes(uniform_noise, -1, -2))
    log_scales = jax.random.uniform(jax.random.fold_in(key, 2), shape[:-1], jnp.float32, jnp.log(low), jnp.log(high))
    scales = jnp.exp(log_scales)
    core_matrix = jnp.eye(BLOCK, dtype=jnp.float32) + offdiag * symmetric
    return scales[..., :, None] * core_matrix * scales[..., None, :]


def draw_owners(key, part):
    column_keys = jax.random.split(jax.random.fold_in(key, 11), NCB)
    orders = jax.vmap(lambda one_key: jax.random.permutation(one_key, BANDS))(column_keys)
    return (orders.T // SLOTS).astype(jnp.int32)


def draw_stat_left(key, part):
    return BLOCK * definite(jax.random.fold_in(key, 21), 1.0, 3.2)


def draw_stat_right(key, part):
    return BLOCK * definite(jax.random.fold_in(key, 31), 1.0, 3.2)


def draw_root_left(key, part):
    return 0.2 * definite(jax.random.fold_in(key, 41), 1.0, 3.2)


def draw_root_right(key, part):
    return 0.2 * definite(jax.random.fold_in(key, 51), 1.0, 3.2)


def plant(drawn, stream_key, low, largest):
    place = [jax.random.randint(jax.random.fold_in(stream_key, axis), (), 0, length) for axis, length in enumerate(drawn.shape)]
    widest = drawn.shape.index(max(drawn.shape))
    neighbour = place[:widest] + [(place[widest] + 1) % drawn.shape[widest]] + place[widest + 1:]
    return drawn.at[tuple(place)].set(low).at[tuple(neighbour)].set(largest)


def levels(key, dims, cuts, low, largest):
    level, own = 1.0, jax.random.fold_in(key, 6)
    for axis_at, blocks in cuts:
        steps = jnp.exp(jax.random.uniform(jax.random.fold_in(own, axis_at), (blocks,), jnp.float32, low / len(cuts), largest / len(cuts)))
        level = level * jnp.repeat(steps, dims[axis_at] // blocks).reshape([-1 if axis == axis_at else 1 for axis in range(len(dims))])
    return level


def split_up(count, total, bound, skew):
    portions = [(1 << 20) // math.isqrt(standing ** skew) + 1 for standing in range(2, count + 1)]
    surplus, holding = total - bound - (count - 1), [1] * (count - 1)
    while surplus > 0:
        candidates = [i for i in range(count - 1) if holding[i] < bound]
        whole, left = sum([portions[i] for i in candidates]), surplus
        for i in candidates:
            extra = min(bound - holding[i], max(1, left * portions[i] // whole), surplus)
            holding[i] = holding[i] + extra
            surplus = surplus - extra
    return np.array([bound] + holding)


def uneven(key, number_of, total, limit, slope):
    if number_of == 2:
        one = jax.random.randint(key, (), max(1, total - limit), min(limit, total - 1) + 1)
        return jnp.stack([one, total - one])
    lengths = jnp.asarray(split_up(number_of, total, limit, slope), jnp.int32)
    couples = (number_of - 1) // 2
    donor, receiver = lengths[1:1 + 2 * couples:2], lengths[2:2 + 2 * couples:2]
    slack = jnp.minimum(donor - 1, limit - receiver)
    moved = jax.random.randint(jax.random.fold_in(key, 1), (couples,), 0, 1 << 20) % (slack + 1)
    lengths = lengths.at[1:1 + 2 * couples:2].set(donor - moved).at[2:2 + 2 * couples:2].set(receiver + moved)
    return lengths[jax.random.permutation(jax.random.fold_in(key, 2), number_of)]


def scatter_about(rng, shape, scale, bound, pieces=(), kind=jnp.bfloat16):
    drawn = jax.random.normal(rng, shape, jnp.float32) * scale
    if len(pieces) > 0:
        drawn = levels(rng, shape, pieces, -0.22, 0.18) * drawn
    return jnp.clip(drawn, min=-bound, max=bound).astype(kind)


def setup_inputs(seed: int = 0) -> dict:
    streams_of = jax.random.split(jax.random.key(seed), 9)
    return {
        "gradient": scatter_about(streams_of[0], (N_FSDP * CAP, COLS), 1.0, 6.0, ((0, 16), (1, 16)), jnp.float32),
        "row_counts": uneven(streams_of[1], N_FSDP, ROWS, CAP, 2).astype(jnp.int32),
        "owners": draw_owners(jax.random.fold_in(streams_of[8], 71), 0),
        "refresh_flags": plant((jax.random.randint(streams_of[3], (BANDS, NCB), 0, 2) < 1).astype(jnp.int32), jax.random.fold_in(streams_of[3], 1), 0, 1),
        "stat_left": draw_stat_left(jax.random.fold_in(streams_of[8], 71), 0),
        "stat_right": draw_stat_right(jax.random.fold_in(streams_of[8], 71), 0),
        "root_left": draw_root_left(jax.random.fold_in(streams_of[8], 71), 0),
        "root_right": draw_root_right(jax.random.fold_in(streams_of[8], 71), 0),
    }


highest = lax.Precision.HIGHEST
stat_decay = 0.9
graft_eps = 1e-06

def matmul(left_part, right_part):
    return jnp.dot(left_part, right_part, precision=highest, preferred_element_type=jnp.float32)

def inverse_root(matrix, sweeps):
    identity = jnp.eye(matrix.shape[0], dtype=jnp.float32)
    scaling = 2.5 / jnp.sqrt(jnp.sum(matrix * matrix))
    current = identity * jnp.sqrt(jnp.sqrt(scaling))
    moment = matrix * scaling
    for sweep_pos in range(sweeps):
        factor = (5.0 * identity - moment) * 0.25
        current = matmul(current, factor)
        if sweep_pos + 1 < sweeps:
            squared = matmul(factor, factor)
            moment = matmul(matmul(squared, squared), moment)
    return current

def tile_update(grad_tile, left_stat, right_stat, old_left, old_right, refresh_now):
    fresh_left = stat_decay * left_stat + (1.0 - stat_decay) * matmul(grad_tile, grad_tile.T)
    fresh_right = stat_decay * right_stat + (1.0 - stat_decay) * matmul(grad_tile.T, grad_tile)
    left_root, right_root = lax.cond(refresh_now > 0, lambda: (inverse_root(fresh_left, ITERS), inverse_root(fresh_right, ITERS)), lambda: (old_left, old_right))
    precond = matmul(matmul(left_root, grad_tile), right_root)
    graft_ratio = jnp.mean(grad_tile * grad_tile) / (jnp.mean(precond * precond) + graft_eps)
    return (fresh_left, fresh_right, (precond * jnp.sqrt(graft_ratio)).astype(jnp.bfloat16))

def slot_table(owners):
    band_count = owners.shape[0]
    same_owner = owners[:, None, :] == owners[None, :, :]
    ordinal = jnp.arange(band_count, dtype=jnp.int32)
    earlier = (ordinal[None, :] < ordinal[:, None])[:, :, None]
    return lax.optimization_barrier(jnp.sum(jnp.where(same_owner & earlier, 1, 0), axis=1)).astype(jnp.int32)

def reference(gradient, row_counts, owners, refresh_flags, stat_left, stat_right, root_left, root_right):
    tile_size = BLOCK
    offsets = (jnp.cumsum(row_counts) - row_counts).astype(jnp.int32)
    local_rows = jnp.arange(CAP, dtype=jnp.int32)
    live_rows = local_rows[None, :] < row_counts[:, None]
    dest_rows = jnp.where(live_rows, offsets[:, None] + local_rows[None, :], ROWS).reshape(-1).astype(jnp.int32)
    dense_grad = jnp.zeros((ROWS, COLS), gradient.dtype).at[dest_rows].set(gradient, mode='drop')
    slot_rank = slot_table(owners)
    holder = (owners * SLOTS + slot_rank).astype(jnp.int32)

    def update_tile(tile_index):
        band_pos = tile_index // NCB
        column_pos = tile_index % NCB
        grad_tile = lax.dynamic_slice(dense_grad, (band_pos * tile_size, column_pos * tile_size), (tile_size, tile_size))
        state_index = holder[band_pos, column_pos]
        return tile_update(grad_tile, stat_left[state_index, column_pos], stat_right[state_index, column_pos], root_left[state_index, column_pos], root_right[state_index, column_pos], refresh_flags[band_pos, column_pos])
    fresh_lefts, fresh_rights, tile_stack = lax.map(update_tile, jnp.arange(BANDS * NCB, dtype=jnp.int32))
    flat_holder = holder.reshape(-1)
    flat_column = jnp.tile(jnp.arange(NCB, dtype=jnp.int32), BANDS)
    new_left = stat_left.at[flat_holder, flat_column].set(fresh_lefts)
    new_right = stat_right.at[flat_holder, flat_column].set(fresh_rights)
    dense_direction = tile_stack.reshape(BANDS, NCB, tile_size, tile_size).transpose(0, 2, 1, 3).reshape(ROWS, COLS)
    source_rows = jnp.clip(offsets[:, None] + local_rows[None, :], 0, ROWS - 1).reshape(-1)
    picked = dense_direction[source_rows]
    direction = jnp.where(live_rows.reshape(-1)[:, None], picked, jnp.zeros_like(picked))
    return (direction, new_left, new_right)
```

```python
import functools

import jax
import jax.numpy as jnp
from jax import lax
from jax.experimental import pallas as pl
from jax.experimental.pallas import tpu as pltpu
from jax.sharding import PartitionSpec as P

ITERS = 3
STAT_DECAY = 0.9
GRAFT_EPS = 1e-06
PAD = 48
LANES = 128


f32 = jnp.float32
bf16 = jnp.bfloat16
SMEM = pl.BlockSpec(memory_space=pltpu.SMEM)
VMEM = pl.BlockSpec(memory_space=pltpu.VMEM)
ANY = pl.BlockSpec(memory_space=pl.ANY)


def params(mib=40):
    return pltpu.CompilerParams(vmem_limit_bytes=mib << 20)


def row_offsets(counts_ref, n):
    offsets = [jnp.int32(0)]
    for g in range(n - 1):
        offsets.append(offsets[-1] + counts_ref[g])
    return offsets


def own_entry(values, me):
    out = values[0]
    for g in range(1, len(values)):
        out = jnp.where(me == g, values[g], out)
    return out


def strips(width):
    return [(t, slice(t * LANES, (t + 1) * LANES)) for t in range(width // LANES)]


def spread_kernel(n, counts_ref, grad_ref, out_ref, lanes):
    me = lax.axis_index("fsdp")
    offset = own_entry(row_offsets(counts_ref, n), me)
    each = grad_ref.shape[0] // n
    for t, lane in strips(grad_ref.shape[1]):
        lanes[t, : each * n, :] = grad_ref[:, lane]
        lanes[t, each * n :, :] = jnp.zeros(((PAD - each) * n, LANES), f32)
    for q in range(n):
        p = (q + offset) & (n - 1)
        for t, lane in strips(grad_ref.shape[1]):
            out_ref[p, :, lane] = lanes[t, pl.ds(q, PAD, stride=n), :]


def collect_kernel(n, counts_ref, owners_ref, in_ref, out_ref, dense):
    me = lax.axis_index("fsdp")
    part = out_ref.shape[1]
    offsets = row_offsets(counts_ref, n)
    for f in range(n):
        start = (offsets[f] + (n - 1) - me) // n
        for t, lane in strips(in_ref.shape[2]):
            dense[t, pl.ds(start, PAD), :] = in_ref[f, :, lane]
    for j in range(n):
        for t, lane in strips(in_ref.shape[2]):
            out_ref[owners_ref[j], :, lane] = dense[t, j * part : (j + 1) * part, :]


def scatter_kernel(n, counts_ref, owners_ref, in_ref, out_ref, dense):
    me = lax.axis_index("fsdp")
    part = in_ref.shape[1]
    for j in range(n):
        for t, lane in strips(in_ref.shape[2]):
            dense[t, j * part : (j + 1) * part, :] = in_ref[owners_ref[j], :, lane].astype(f32)
    dense[:, n * part :, :] = jnp.zeros((dense.shape[0], PAD, LANES), f32)
    offsets = row_offsets(counts_ref, n)
    for f in range(n):
        start = (offsets[f] + (n - 1) - me) // n
        for t, lane in strips(in_ref.shape[2]):
            out_ref[f, :, lane] = dense[t, pl.ds(start, PAD), :].astype(bf16)


def merge_kernel(n, counts_ref, in_ref, first_ref, second_ref, slab):
    me = lax.axis_index("fsdp")
    offset = own_entry(row_offsets(counts_ref, n), me)
    live = own_entry([counts_ref[g] for g in range(n)], me)
    for q in range(n):
        p = (q + offset) & (n - 1)
        for t, lane in strips(in_ref.shape[2]):
            slab[t, pl.ds(q, PAD, stride=n), :] = in_ref[p, :, lane].astype(f32)
    half = first_ref.shape[0]
    for at, out_ref in ((0, first_ref), (half, second_ref)):
        rows = at + lax.broadcasted_iota(jnp.int32, (half, LANES), 0)
        for t, lane in strips(out_ref.shape[1]):
            picked = slab[t, at : at + half, :]
            out_ref[:, lane] = jnp.where(rows < live, picked, 0.0).astype(bf16)


def split(x):
    high = x.astype(bf16)
    return high, (x - high.astype(f32)).astype(bf16)


def update_kernel(
    n, owners_ref, flags_ref, in_ref, sl_hbm, sr_hbm, rl_hbm, rr_hbm,
    nl_hbm, nr_hbm, out_ref,
    grad, stats, roots, high, low, total, sems,
):
    me = lax.axis_index("fsdp")
    size = grad.shape[1]
    part = in_ref.shape[1]
    GRAD, GRAD_T, FIRST, ONE, TWO, ROOT = 0, 1, 2, 4, 6, 8

    def load(hbm, ref, at):
        return pltpu.make_async_copy(hbm.at[0, 0], ref, sems.at[at])

    loads = [
        load(sl_hbm, stats.at[0], 0), load(sr_hbm, stats.at[1], 1),
        load(rl_hbm, roots.at[0], 2), load(rr_hbm, roots.at[1], 3),
    ]
    for one in loads:
        one.start()

    refresh = jnp.int32(0)
    for j in range(n):
        refresh = jnp.where(owners_ref[j] == me, flags_ref[j], refresh)

    def put(at, x):
        top, rest = split(x)
        high[at] = top
        low[at] = rest

    def mm(left, right):
        lh, ll = high[left], low[left]
        rh, rl = high[right], low[right]
        return jnp.dot(
            jnp.concatenate([lh, lh, ll], axis=1),
            jnp.concatenate([rh, rl, rh], axis=0),
            preferred_element_type=f32,
        )

    for p in range(n):
        for t, lane in strips(size):
            grad[t, pl.ds(p, part, stride=n), :] = in_ref[p, :, lane]
    whole = jnp.concatenate([grad[t] for t, _ in strips(size)], axis=1)
    put(GRAD, whole)
    put(GRAD_T, whole.T)
    grad_square = jnp.sum(whole * whole)

    loads[0].wait()
    loads[1].wait()

    def statistics(side, carry):
        product = mm(GRAD + side, GRAD_T - side)
        stats[side] = STAT_DECAY * stats[side] + (1.0 - STAT_DECAY) * product
        return carry

    lax.fori_loop(0, 2, statistics, 0)
    stores = [
        pltpu.make_async_copy(stats.at[0], nl_hbm.at[0, 0], sems.at[4]),
        pltpu.make_async_copy(stats.at[1], nr_hbm.at[0, 0], sems.at[5]),
    ]
    for one in stores:
        one.start()
    loads[2].wait()
    loads[3].wait()

    @pl.when(refresh > 0)
    def _():
        row = lax.broadcasted_iota(jnp.int32, (size, size), 0)
        col = lax.broadcasted_iota(jnp.int32, (size, size), 1)

        def factor(moment):
            return (jnp.where(row == col, 5.0, 0.0) - moment) * 0.25

        def one_root(side, carry):
            matrix = stats[side]
            scaling = 2.5 / jnp.sqrt(jnp.full((1, 1), jnp.sum(matrix * matrix), f32))
            moment = matrix * scaling
            put(FIRST, moment)
            put(ONE, factor(moment))
            put(TWO, mm(ONE, ONE))
            put(TWO + 1, mm(TWO, TWO))
            moment = mm(TWO + 1, FIRST)
            put(FIRST, moment)
            put(ONE + 1, factor(moment))
            put(FIRST + 1, mm(ONE, ONE + 1))
            put(TWO, mm(ONE + 1, ONE + 1))
            put(TWO + 1, mm(TWO, TWO))
            put(TWO, factor(mm(TWO + 1, FIRST)))
            put(ROOT + side, mm(FIRST + 1, TWO) * jnp.sqrt(jnp.sqrt(scaling)))
            return carry

        lax.fori_loop(0, 2, one_root, 0)

    @pl.when(refresh <= 0)
    def _():
        for side in range(2):
            put(ROOT + side, roots[side])

    put(FIRST, mm(ROOT, GRAD))
    precond = mm(FIRST, ROOT + 1)
    for t, lane in strips(size):
        total[t] = precond[:, lane]
    count = float(size * size)
    ratio = (grad_square / count) / (jnp.sum(precond * precond) / count + GRAFT_EPS)
    scale = jnp.sqrt(jnp.full((1, 1), ratio, f32))
    for p in range(n):
        for t, lane in strips(size):
            picked = total[t, pl.ds(p, part, stride=n), :]
            out_ref[p, :, lane] = (picked * scale).astype(bf16)
    for one in stores:
        one.wait()


def place_kernel(columns_of, rows_of, width, *refs):
    pieces, out_ref, sems = refs[: len(columns_of)], refs[-2], refs[-1]
    me = lax.axis_index("rep")
    copies = []
    for at, piece in enumerate(pieces):
        start = pl.multiple_of(columns_of[at](me) * width, width)
        copies.append(
            pltpu.make_async_copy(
                piece,
                out_ref.at[pl.ds(rows_of[at], piece.shape[0]), pl.ds(start, width)],
                sems.at[at],
            )
        )
    for one in copies:
        one.start()
    for one in copies:
        one.wait()


def place(out, shape, entries):
    pieces = [e[0] for e in entries]
    width = pieces[0].shape[1]
    kernel = functools.partial(
        place_kernel, [e[2] for e in entries], [e[1] for e in entries], width
    )
    more = [] if out is None else [out]
    return pl.pallas_call(
        kernel,
        out_shape=jax.ShapeDtypeStruct(shape, pieces[0].dtype),
        in_specs=[ANY] * (len(pieces) + len(more)),
        out_specs=ANY,
        scratch_shapes=[pltpu.SemaphoreType.DMA((len(pieces),))],
        input_output_aliases={len(pieces): 0} if more else {},
        compiler_params=params(16),
    )(*pieces, *more)


def gather_columns(halves, rep):
    rows, width = halves[0].shape
    chips = rep // 2
    shape = (2 * rows, rep * width)

    def perm(step):
        return [(z * 2 + c, ((z + step) % chips) * 2 + c) for z in range(chips) for c in range(2)]

    swap = [(r, r ^ 1) for r in range(rep)]

    def column(step, other):
        def of(me):
            return lax.rem(me // 2 + chips - step, chips) * 2 + ((me & 1) ^ other)
        return of

    def both(half, at, step):
        return [
            (half, at, column(step, 0)),
            (lax.ppermute(half, "rep", swap), at, column(step, 1)),
        ]

    hops = chips // 2
    out = None
    ahead, behind = list(halves), list(halves)
    entries = both(halves[0], 0, 0) + both(halves[1], rows, 0)
    for step in range(1, hops + 1):
        last = step == hops
        moved = []
        for k in range(2):
            if not last or k == 0:
                ahead[k] = lax.ppermute(ahead[k], "rep", perm(1))
                moved.append((ahead[k], k * rows, step))
            if not last or k == 1:
                behind[k] = lax.ppermute(behind[k], "rep", perm(-1))
                moved.append((behind[k], k * rows, chips - step))
        out = place(out, shape, entries)
        entries = []
        for piece, at, distance in moved:
            entries += both(piece, at, distance)
    return place(out, shape, entries)


def per_device(n, rep, gradient, row_counts, owners, refresh_flags, stat_left, stat_right, root_left, root_right):
    capacity, width = gradient.shape
    tile = stat_left.shape[-1]
    part = tile // n
    owners = owners.reshape(-1)
    flags = refresh_flags.reshape(-1)
    struct = jax.ShapeDtypeStruct

    def lanes_of(rows):
        return pltpu.VMEM((width // LANES, rows, LANES), f32)

    sent = pl.pallas_call(
        functools.partial(spread_kernel, n),
        out_shape=struct((n, PAD, width), f32),
        in_specs=[SMEM, VMEM], out_specs=VMEM,
        scratch_shapes=[lanes_of(n * PAD)],
        compiler_params=params(),
    )(row_counts, gradient)
    mine = lax.all_to_all(sent, "fsdp", 0, 0, tiled=True)
    sent = pl.pallas_call(
        functools.partial(collect_kernel, n),
        out_shape=struct((n, part, width), f32),
        in_specs=[SMEM, SMEM, VMEM], out_specs=VMEM,
        scratch_shapes=[lanes_of(tile + PAD)],
        compiler_params=params(),
    )(row_counts, owners, mine)
    block = lax.all_to_all(sent, "fsdp", 0, 0, tiled=True)
    square = (tile, tile)
    new_left, new_right, tiles = pl.pallas_call(
        functools.partial(update_kernel, n),
        out_shape=(
            struct(stat_left.shape, f32), struct(stat_right.shape, f32),
            struct((n, part, width), bf16),
        ),
        in_specs=[SMEM, SMEM, VMEM, ANY, ANY, ANY, ANY],
        out_specs=(ANY, ANY, VMEM),
        scratch_shapes=[
            lanes_of(tile), pltpu.VMEM((2,) + square, f32), pltpu.VMEM((2,) + square, f32),
            pltpu.VMEM((10,) + square, bf16), pltpu.VMEM((10,) + square, bf16),
            lanes_of(tile), pltpu.SemaphoreType.DMA((6,)),
        ],
        compiler_params=params(48),
    )(owners, flags, block, stat_left, stat_right, root_left, root_right)
    mine = lax.all_to_all(tiles, "fsdp", 0, 0, tiled=True)
    sent = pl.pallas_call(
        functools.partial(scatter_kernel, n),
        out_shape=struct((n, PAD, width), bf16),
        in_specs=[SMEM, SMEM, VMEM], out_specs=VMEM,
        scratch_shapes=[lanes_of(tile + PAD)],
        compiler_params=params(),
    )(row_counts, owners, mine)
    rows = lax.all_to_all(sent, "fsdp", 0, 0, tiled=True)
    half = struct((capacity // 2, width), bf16)
    halves = pl.pallas_call(
        functools.partial(merge_kernel, n),
        out_shape=(half, half),
        in_specs=[SMEM, VMEM], out_specs=(VMEM, VMEM),
        scratch_shapes=[lanes_of(n * PAD)],
        compiler_params=params(),
    )(row_counts, rows)
    direction = gather_columns(halves, rep)
    return direction, new_left, new_right


def solution(mesh):
    state = P("fsdp", "rep", None, None)
    return jax.shard_map(
        functools.partial(per_device, mesh.shape["fsdp"], mesh.shape["rep"]),
        mesh=mesh,
        in_specs=(P("fsdp", "rep"), P(), P(None, "rep"), P(None, "rep"), state, state, state, state),
        out_specs=(P("fsdp", None), state, state),
        check_vma=False,
    )
```

```python
import functools

import jax
import jax.numpy as jnp
from jax import lax
from jax.experimental import pallas as pl
from jax.experimental.pallas import tpu as pltpu
from jax.sharding import PartitionSpec as P

ITERS = 3
STAT_DECAY = 0.9
GRAFT_EPS = 1e-06
PAD = 48
LANES = 128


f32 = jnp.float32
bf16 = jnp.bfloat16
SMEM = pl.BlockSpec(memory_space=pltpu.SMEM)
VMEM = pl.BlockSpec(memory_space=pltpu.VMEM)
ANY = pl.BlockSpec(memory_space=pl.ANY)


def params(mib=14):
    return pltpu.CompilerParams(vmem_limit_bytes=mib << 20)


def row_offsets(counts_ref, n):
    offsets = [jnp.int32(0)]
    for g in range(n - 1):
        offsets.append(offsets[-1] + counts_ref[g])
    return offsets


def own_entry(values, me):
    out = values[0]
    for g in range(1, len(values)):
        out = jnp.where(me == g, values[g], out)
    return out


def strips(width):
    return [(t, slice(t * LANES, (t + 1) * LANES)) for t in range(width // LANES)]


def spread_kernel(n, table_ref, grad_ref, out_ref, lanes, sems):
    me = lax.axis_index("fsdp")
    offset = own_entry(row_offsets(table_ref, n), me)
    rows = grad_ref.shape[0]
    each = rows // n
    loads = [
        pltpu.make_async_copy(grad_ref.at[:, lane], lanes.at[t, pl.ds(0, rows), :], sems.at[t])
        for t, lane in strips(grad_ref.shape[1])
    ]
    for one in loads:
        one.start()
    lanes[:, rows:, :] = jnp.zeros((lanes.shape[0], lanes.shape[1] - rows, LANES), f32)
    for one in loads:
        one.wait()
    for q in range(n):
        p = (q + offset) & (n - 1)
        for t, _ in strips(grad_ref.shape[1]):
            picked = lanes[t, pl.ds(q, PAD, stride=n), :]
            out_ref[p, t * each : (t + 1) * each, :] = picked[:each, :]


def collect_kernel(n, table_ref, in_ref, out_ref, dense):
    me = lax.axis_index("fsdp")
    part, width = out_ref.shape[1:]
    each = in_ref.shape[1] // (width // LANES)
    offsets = row_offsets(table_ref, n)
    for f in range(n):
        start = (offsets[f] + (n - 1) - me) // n
        for t, lane in strips(width):
            dense[t, pl.ds(start, each), :] = in_ref[f, t * each : (t + 1) * each, :]
    for j in range(n):
        for t, lane in strips(width):
            out_ref[table_ref[n + j], :, lane] = dense[t, j * part : (j + 1) * part, :]


def scatter_kernel(n, table_ref, in_ref, out_ref, dense, stage):
    me = lax.axis_index("fsdp")
    part, width = in_ref.shape[1:]
    each = out_ref.shape[1] // (width // LANES)
    for j in range(n):
        for t, lane in strips(width):
            dense[t, j * part : (j + 1) * part, :] = in_ref[table_ref[n + j], :, lane].astype(f32)
    dense[:, n * part :, :] = jnp.zeros((dense.shape[0], PAD, LANES), f32)
    offsets = row_offsets(table_ref, n)
    for f in range(n):
        start = (offsets[f] + (n - 1) - me) // n
        for t, _ in strips(width):
            stage[f, t * each : (t + 1) * each, :] = dense[t, pl.ds(start, each), :]
    for f in range(n):
        out_ref[f] = stage[f].astype(bf16)


def merge_kernel(n, table_ref, in_ref, first_ref, second_ref, stage, slab):
    me = lax.axis_index("fsdp")
    offset = own_entry(row_offsets(table_ref, n), me)
    live = own_entry([table_ref[g] for g in range(n)], me)
    half, width = first_ref.shape
    each = 2 * half // n
    for p in range(n):
        stage[p] = in_ref[p].astype(f32)
    for q in range(n):
        p = (q + offset) & (n - 1)
        for t, _ in strips(width):
            slab[t, pl.ds(q, each, stride=n), :] = stage[p, t * each : (t + 1) * each, :]
    for at, out_ref in ((0, first_ref), (half, second_ref)):
        ids = at + lax.broadcasted_iota(jnp.int32, (half, LANES), 0)
        for t, lane in strips(width):
            picked = slab[t, at : at + half, :]
            out_ref[:, lane] = jnp.where(ids < live, picked, 0.0).astype(bf16)


def split(x):
    high = x.astype(bf16)
    return high, (x - high.astype(f32)).astype(bf16)


def update_kernel(
    n, table_ref, in_ref, sl_hbm, sr_hbm, rl_hbm, rr_hbm,
    nl_hbm, nr_hbm, out_ref,
    grad, stats, roots, high, low, total, sems,
):
    me = lax.axis_index("fsdp")
    size = grad.shape[1]
    part = in_ref.shape[1]
    GRAD, GRAD_T, FIRST, ONE, TWO, ROOT = 0, 1, 2, 4, 6, 8

    def load(hbm, ref, at):
        return pltpu.make_async_copy(hbm.at[0, 0], ref, sems.at[at])

    loads = [
        load(sl_hbm, stats.at[0], 0), load(sr_hbm, stats.at[1], 1),
        load(rl_hbm, roots.at[0], 2), load(rr_hbm, roots.at[1], 3),
    ]
    for one in loads:
        one.start()

    refresh = jnp.int32(0)
    for j in range(n):
        refresh = jnp.where(table_ref[n + j] == me, table_ref[2 * n + j], refresh)

    def put(at, x):
        top, rest = split(x)
        high[at] = top
        low[at] = rest

    def mm(left, right):
        lh, ll = high[left], low[left]
        rh, rl = high[right], low[right]
        return jnp.dot(
            jnp.concatenate([lh, lh, ll], axis=1),
            jnp.concatenate([rh, rl, rh], axis=0),
            preferred_element_type=f32,
        )

    for p in range(n):
        for t, lane in strips(size):
            grad[t, pl.ds(p, part, stride=n), :] = in_ref[p, :, lane]
    whole = jnp.concatenate([grad[t] for t, _ in strips(size)], axis=1)
    put(GRAD, whole)
    put(GRAD_T, whole.T)
    grad_square = jnp.sum(whole * whole)

    loads[0].wait()
    loads[1].wait()

    def statistics(side, carry):
        product = mm(GRAD + side, GRAD_T - side)
        stats[side] = STAT_DECAY * stats[side] + (1.0 - STAT_DECAY) * product
        return carry

    lax.fori_loop(0, 2, statistics, 0)
    stores = [
        pltpu.make_async_copy(stats.at[0], nl_hbm.at[0, 0], sems.at[4]),
        pltpu.make_async_copy(stats.at[1], nr_hbm.at[0, 0], sems.at[5]),
    ]
    for one in stores:
        one.start()
    loads[2].wait()
    loads[3].wait()

    @pl.when(refresh > 0)
    def _():
        row = lax.broadcasted_iota(jnp.int32, (size, size), 0)
        col = lax.broadcasted_iota(jnp.int32, (size, size), 1)

        def factor(moment):
            return (jnp.where(row == col, 5.0, 0.0) - moment) * 0.25

        def one_root(side, carry):
            matrix = stats[side]
            scaling = 2.5 / jnp.sqrt(jnp.full((1, 1), jnp.sum(matrix * matrix), f32))
            moment = matrix * scaling
            put(FIRST, moment)
            put(ONE, factor(moment))
            put(TWO, mm(ONE, ONE))
            put(TWO + 1, mm(TWO, TWO))
            moment = mm(TWO + 1, FIRST)
            put(FIRST, moment)
            put(ONE + 1, factor(moment))
            put(FIRST + 1, mm(ONE, ONE + 1))
            put(TWO, mm(ONE + 1, ONE + 1))
            put(TWO + 1, mm(TWO, TWO))
            put(TWO, factor(mm(TWO + 1, FIRST)))
            put(ROOT + side, mm(FIRST + 1, TWO) * jnp.sqrt(jnp.sqrt(scaling)))
            return carry

        lax.fori_loop(0, 2, one_root, 0)

    @pl.when(refresh <= 0)
    def _():
        for side in range(2):
            put(ROOT + side, roots[side])

    put(FIRST, mm(ROOT, GRAD))
    precond = mm(FIRST, ROOT + 1)
    for t, lane in strips(size):
        total[t] = precond[:, lane]
    count = float(size * size)
    ratio = (grad_square / count) / (jnp.sum(precond * precond) / count + GRAFT_EPS)
    scale = jnp.sqrt(jnp.full((1, 1), ratio, f32))
    for p in range(n):
        for t, lane in strips(size):
            picked = total[t, pl.ds(p, part, stride=n), :]
            out_ref[p, :, lane] = (picked * scale).astype(bf16)
    for one in stores:
        one.wait()


def place_kernel(places, width, *refs):
    pieces, out_ref, sems = refs[: len(places)], refs[-2], refs[-1]
    me = lax.axis_index("rep")
    copies = []
    for at, (row, column) in enumerate(places):
        start = pl.multiple_of(column(me) * width, width)
        target = out_ref.at[pl.ds(row, pieces[at].shape[0]), pl.ds(start, width)]
        copies.append(pltpu.make_async_copy(pieces[at], target, sems.at[at]))
    for one in copies:
        one.start()
    for one in copies:
        one.wait()


def place(out, shape, entries):
    pieces = [e[0] for e in entries]
    kernel = functools.partial(place_kernel, [e[1:] for e in entries], pieces[0].shape[1])
    more = [] if out is None else [out]
    return pl.pallas_call(
        kernel,
        out_shape=jax.ShapeDtypeStruct(shape, pieces[0].dtype),
        in_specs=[ANY] * (len(pieces) + len(more)),
        out_specs=ANY,
        scratch_shapes=[pltpu.SemaphoreType.DMA((len(pieces),))],
        input_output_aliases={len(pieces): 0} if more else {},
        compiler_params=params(16),
    )(*pieces, *more)


def gather_columns(halves, rep):
    half, width = halves[0].shape
    shape = (2 * half, rep * width)
    chips = rep // 2
    hops = chips // 2

    def hop(piece, step):
        pairs = [(z * 2 + c, ((z + step) % chips) * 2 + c) for z in range(chips) for c in range(2)]
        return lax.ppermute(piece, "rep", pairs)

    def entries(piece, which, step):
        def column(other):
            def of(me):
                return lax.rem(me // 2 + chips - step, chips) * 2 + ((me & 1) ^ other)
            return of

        swapped = lax.ppermute(piece, "rep", [(r, r ^ 1) for r in range(rep)])
        return [(piece, which * half, column(0)), (swapped, which * half, column(1))]

    out, waiting = None, []
    moving = [[halves[0]], [halves[1]]]
    for step in range(hops + 1):
        for which in range(2):
            pieces = moving[which]
            if out is not None:
                *pieces, out = lax.optimization_barrier((*pieces, out))
            if step == 0:
                moving[which] = [hop(pieces[0], 1), hop(pieces[0], -1)]
                froms = [0]
            elif step < hops:
                keep = (True, True) if step + 1 < hops else (which == 0, which == 1)
                moving[which] = [hop(p, d) for p, d, k in zip(pieces, (1, -1), keep) if k]
                froms = [step, chips - step]
            else:
                froms = [hops]
            if waiting:
                out = place(out, shape, waiting)
            waiting = []
            for piece, distance in zip(pieces, froms):
                waiting += entries(piece, which, distance)
    return place(out, shape, waiting)


def per_device(n, rep, gradient, row_counts, owners, refresh_flags, stat_left, stat_right, root_left, root_right):
    capacity, width = gradient.shape
    tile = stat_left.shape[-1]
    part, each, many = tile // n, capacity // n, width // LANES
    struct = jax.ShapeDtypeStruct

    def in_hbm(x):
        return pltpu.with_memory_space_constraint(x, pltpu.HBM)

    states = [in_hbm(x) for x in (stat_left, stat_right, root_left, root_right)]
    table = jnp.concatenate([row_counts, owners.reshape(-1), refresh_flags.reshape(-1)])

    def rows_of(count, strip_count=many):
        return pltpu.VMEM((strip_count, count, LANES), f32)

    def exchange(x):
        return lax.all_to_all(x, "fsdp", 0, 0, tiled=True)

    sent = pl.pallas_call(
        functools.partial(spread_kernel, n),
        out_shape=struct((n, many * each, LANES), f32),
        in_specs=[SMEM, ANY], out_specs=VMEM,
        scratch_shapes=[rows_of(n * PAD), pltpu.SemaphoreType.DMA((many,))],
        compiler_params=params(),
    )(table, in_hbm(gradient))
    sent = pl.pallas_call(
        functools.partial(collect_kernel, n),
        out_shape=struct((n, part, width), f32),
        in_specs=[SMEM, VMEM], out_specs=VMEM,
        scratch_shapes=[rows_of(tile + PAD)],
        compiler_params=params(),
    )(table, exchange(sent))
    square = (tile, tile)
    new_left, new_right, tiles = pl.pallas_call(
        functools.partial(update_kernel, n),
        out_shape=(struct(stat_left.shape, f32), struct(stat_right.shape, f32))
        + (struct((n, part, width), bf16),),
        in_specs=[SMEM, VMEM, ANY, ANY, ANY, ANY],
        out_specs=(ANY, ANY, VMEM),
        scratch_shapes=[
            rows_of(tile), pltpu.VMEM((2,) + square, f32), pltpu.VMEM((2,) + square, f32),
            pltpu.VMEM((10,) + square, bf16), pltpu.VMEM((10,) + square, bf16),
            rows_of(tile), pltpu.SemaphoreType.DMA((6,)),
        ],
        compiler_params=params(36),
    )(table, exchange(sent), *states)

    sent = pl.pallas_call(
        functools.partial(scatter_kernel, n),
        out_shape=struct((n, many * each, LANES), bf16),
        in_specs=[SMEM, VMEM], out_specs=VMEM,
        scratch_shapes=[rows_of(tile + PAD), rows_of(many * each, n)],
        compiler_params=params(),
    )(table, exchange(tiles))
    half = struct((capacity // 2, width), bf16)
    halves = pl.pallas_call(
        functools.partial(merge_kernel, n),
        out_shape=(half, half),
        in_specs=[SMEM, VMEM], out_specs=(VMEM, VMEM),
        scratch_shapes=[rows_of(many * each, n), rows_of(n * PAD)],
        compiler_params=params(),
    )(table, exchange(sent))
    return gather_columns(halves, rep), new_left, new_right


def solution(mesh):
    state = P("fsdp", "rep", None, None)
    return jax.shard_map(
        functools.partial(per_device, mesh.shape["fsdp"], mesh.shape["rep"]),
        mesh=mesh,
        in_specs=(P("fsdp", "rep"), P(), P(None, "rep"), P(None, "rep"), state, state, state, state),
        out_specs=(P("fsdp", None), state, state),
        check_vma=False,
    )
```

```python
import functools

import jax
import jax.numpy as jnp
from jax import lax
from jax.experimental import pallas as pl
from jax.experimental.pallas import tpu as pltpu
from jax.sharding import PartitionSpec as P

ITERS = 3
STAT_DECAY = 0.9
GRAFT_EPS = 1e-06
PAD = 48
LANES = 128


f32 = jnp.float32
bf16 = jnp.bfloat16
SMEM = pl.BlockSpec(memory_space=pltpu.SMEM)
VMEM = pl.BlockSpec(memory_space=pltpu.VMEM)
ANY = pl.BlockSpec(memory_space=pl.ANY)


def params(mib=16):
    return pltpu.CompilerParams(vmem_limit_bytes=mib << 20)


def row_offsets(counts_ref, n):
    offsets = [jnp.int32(0)]
    for g in range(n - 1):
        offsets.append(offsets[-1] + counts_ref[g])
    return offsets


def own_entry(values, me):
    out = values[0]
    for g in range(1, len(values)):
        out = jnp.where(me == g, values[g], out)
    return out


def strips(width):
    return [(t, slice(t * LANES, (t + 1) * LANES)) for t in range(width // LANES)]


def exponent_of(values):
    peak = jnp.full((1, 1), jnp.max(jnp.abs(values)), f32)
    return jnp.floor(jnp.log2(jnp.maximum(peak, 1e-30))) + 1.0


def encode(values, exponent):
    top = float(2**23 - 1)
    scaled = jnp.round(values * jnp.exp2(23.0 - exponent))
    code = jnp.clip(scaled, -top, top).astype(jnp.int32)
    return code >> 8, code & 255


def join(first, second):
    return (first | (second << 8)) - 32768


def part_of(word):
    word = word + 32768
    return word & 255, word >> 8


def decode(high, low, exponent):
    return (high * 256 + low).astype(f32) * jnp.exp2(exponent - 23.0)


def spread_kernel(n, table_ref, grad_ref, out_ref, lanes, stage, sems):
    me = lax.axis_index("fsdp")
    offset = own_entry(row_offsets(table_ref, n), me)
    rows = grad_ref.shape[0]
    each = rows // n
    loads = [
        pltpu.make_async_copy(grad_ref.at[:, lane], lanes.at[t, pl.ds(0, rows), :], sems.at[t])
        for t, lane in strips(grad_ref.shape[1])
    ]
    for one in loads:
        one.start()
    lanes[:, rows:, :] = jnp.zeros((lanes.shape[0], lanes.shape[1] - rows, LANES), f32)
    for one in loads:
        one.wait()
    exponent = exponent_of(lanes[...])
    many = stage.shape[1]
    for q in range(n):
        p = (q + offset) & (n - 1)
        for t, _ in strips(grad_ref.shape[1]):
            picked = lanes[t, pl.ds(q, PAD, stride=n), :]
            stage[p, t * each : (t + 1) * each, :] = picked[:each, :]
    tail = jnp.broadcast_to(exponent.astype(jnp.int32), (8, LANES))
    for p in range(n):
        high, low = encode(stage[p], exponent)
        out_ref[p, :many, :] = high.astype(jnp.int16)
        rest = jnp.concatenate([join(low[: many // 2], low[many // 2 :]), tail], axis=0)
        out_ref[p, many:, :] = rest.astype(jnp.int16)


def collect_kernel(n, width, table_ref, in_ref, out_ref, stage, dense):
    me = lax.axis_index("fsdp")
    many = stage.shape[1]
    each = many // (width // LANES)
    part = (dense.shape[1] - PAD) // n
    offsets = row_offsets(table_ref, n)
    for f in range(n):
        word = in_ref[f].astype(jnp.int32)
        low = jnp.concatenate(part_of(word[many : many + many // 2]), axis=0)
        exponent = word[many + many // 2 :][:1, :1].astype(f32)
        stage[f] = decode(word[:many], low, exponent)
    for f in range(n):
        start = (offsets[f] + (n - 1) - me) // n
        for t, _ in strips(width):
            dense[t, pl.ds(start, each), :] = stage[f, t * each : (t + 1) * each, :]
    exponent = exponent_of(dense[:, : n * part, :])
    tail = jnp.broadcast_to(exponent.astype(jnp.int32), (16, LANES)).astype(jnp.int16)
    count = width // LANES
    for j in range(n):
        owner = table_ref[n + j]
        lows = []
        for t, _ in strips(width):
            high, low = encode(dense[t, j * part : (j + 1) * part, :], exponent)
            out_ref[owner, t * part : (t + 1) * part, :] = high.astype(jnp.int16)
            lows.append(low)
        for t in range(0, count, 2):
            at = (count + t // 2) * part
            out_ref[owner, at : at + part, :] = join(lows[t], lows[t + 1]).astype(jnp.int16)
        out_ref[owner, count * part * 3 // 2 :, :] = tail


def scatter_kernel(n, table_ref, in_ref, out_ref, dense, stage):
    me = lax.axis_index("fsdp")
    part, width = in_ref.shape[1:]
    each = out_ref.shape[1] // (width // LANES)
    for j in range(n):
        for t, lane in strips(width):
            dense[t, j * part : (j + 1) * part, :] = in_ref[table_ref[n + j], :, lane].astype(f32)
    dense[:, n * part :, :] = jnp.zeros((dense.shape[0], PAD, LANES), f32)
    offsets = row_offsets(table_ref, n)
    for f in range(n):
        start = (offsets[f] + (n - 1) - me) // n
        for t, _ in strips(width):
            stage[f, t * each : (t + 1) * each, :] = dense[t, pl.ds(start, each), :]
    for f in range(n):
        out_ref[f] = stage[f].astype(bf16)


def merge_kernel(n, table_ref, in_ref, first_ref, second_ref, stage, slab):
    me = lax.axis_index("fsdp")
    offset = own_entry(row_offsets(table_ref, n), me)
    live = own_entry([table_ref[g] for g in range(n)], me)
    half, width = first_ref.shape
    each = 2 * half // n
    for p in range(n):
        stage[p] = in_ref[p].astype(f32)
    for q in range(n):
        p = (q + offset) & (n - 1)
        for t, _ in strips(width):
            slab[t, pl.ds(q, each, stride=n), :] = stage[p, t * each : (t + 1) * each, :]
    for at, out_ref in ((0, first_ref), (half, second_ref)):
        ids = at + lax.broadcasted_iota(jnp.int32, (half, LANES), 0)
        for t, lane in strips(width):
            picked = slab[t, at : at + half, :]
            out_ref[:, lane] = jnp.where(ids < live, picked, 0.0).astype(bf16)


def split(x):
    high = x.astype(bf16)
    return high, (x - high.astype(f32)).astype(bf16)


def update_kernel(
    n, table_ref, in_ref, sl_hbm, sr_hbm, rl_hbm, rr_hbm,
    nl_hbm, nr_hbm, out_ref,
    grad, stats, roots, high, low, total, sems,
):
    me = lax.axis_index("fsdp")
    size = grad.shape[1]
    part = size // n
    GRAD, GRAD_T, FIRST, ONE, TWO, ROOT = 0, 1, 2, 4, 6, 8

    def load(hbm, ref, at):
        return pltpu.make_async_copy(hbm.at[0, 0], ref, sems.at[at])

    loads = [
        load(sl_hbm, stats.at[0], 0), load(sr_hbm, stats.at[1], 1),
        load(rl_hbm, roots.at[0], 2), load(rr_hbm, roots.at[1], 3),
    ]
    for one in loads:
        one.start()

    refresh = jnp.int32(0)
    for j in range(n):
        refresh = jnp.where(table_ref[n + j] == me, table_ref[2 * n + j], refresh)

    def put(at, x):
        top, rest = split(x)
        high[at] = top
        low[at] = rest

    def mm(left, right):
        lh, ll = high[left], low[left]
        rh, rl = high[right], low[right]
        return jnp.dot(
            jnp.concatenate([lh, lh, ll], axis=1),
            jnp.concatenate([rh, rl, rh], axis=0),
            preferred_element_type=f32,
        )

    strip_count = size // LANES
    for p in range(n):
        word = in_ref[p].astype(jnp.int32)
        exponent = word[strip_count * part * 3 // 2 :][:1, :1].astype(f32)
        lows = []
        for t in range(strip_count // 2):
            at = (strip_count + t) * part
            lows += part_of(word[at : at + part])
        for t in range(strip_count):
            value = decode(word[t * part : (t + 1) * part], lows[t], exponent)
            grad[t, pl.ds(p, part, stride=n), :] = value
    whole = jnp.concatenate([grad[t] for t, _ in strips(size)], axis=1)
    put(GRAD, whole)
    put(GRAD_T, whole.T)
    grad_square = jnp.sum(whole * whole)

    loads[0].wait()
    loads[1].wait()

    def statistics(side, carry):
        product = mm(GRAD + side, GRAD_T - side)
        stats[side] = STAT_DECAY * stats[side] + (1.0 - STAT_DECAY) * product
        return carry

    lax.fori_loop(0, 2, statistics, 0)
    stores = [
        pltpu.make_async_copy(stats.at[0], nl_hbm.at[0, 0], sems.at[4]),
        pltpu.make_async_copy(stats.at[1], nr_hbm.at[0, 0], sems.at[5]),
    ]
    for one in stores:
        one.start()
    loads[2].wait()
    loads[3].wait()

    @pl.when(refresh > 0)
    def _():
        row = lax.broadcasted_iota(jnp.int32, (size, size), 0)
        col = lax.broadcasted_iota(jnp.int32, (size, size), 1)

        def factor(moment):
            return (jnp.where(row == col, 5.0, 0.0) - moment) * 0.25

        def one_root(side, carry):
            matrix = stats[side]
            scaling = 2.5 / jnp.sqrt(jnp.full((1, 1), jnp.sum(matrix * matrix), f32))
            moment = matrix * scaling
            put(FIRST, moment)
            put(ONE, factor(moment))
            put(TWO, mm(ONE, ONE))
            put(TWO + 1, mm(TWO, TWO))
            moment = mm(TWO + 1, FIRST)
            put(FIRST, moment)
            put(ONE + 1, factor(moment))
            put(FIRST + 1, mm(ONE, ONE + 1))
            put(TWO, mm(ONE + 1, ONE + 1))
            put(TWO + 1, mm(TWO, TWO))
            put(TWO, factor(mm(TWO + 1, FIRST)))
            put(ROOT + side, mm(FIRST + 1, TWO) * jnp.sqrt(jnp.sqrt(scaling)))
            return carry

        lax.fori_loop(0, 2, one_root, 0)

    @pl.when(refresh <= 0)
    def _():
        for side in range(2):
            put(ROOT + side, roots[side])

    put(FIRST, mm(ROOT, GRAD))
    precond = mm(FIRST, ROOT + 1)
    for t, lane in strips(size):
        total[t] = precond[:, lane]
    count = float(size * size)
    ratio = (grad_square / count) / (jnp.sum(precond * precond) / count + GRAFT_EPS)
    scale = jnp.sqrt(jnp.full((1, 1), ratio, f32))
    for p in range(n):
        for t, lane in strips(size):
            picked = total[t, pl.ds(p, part, stride=n), :]
            out_ref[p, :, lane] = (picked * scale).astype(bf16)
    for one in stores:
        one.wait()


def place_kernel(places, width, *refs):
    pieces, out_ref, sems = refs[: len(places)], refs[-2], refs[-1]
    me = lax.axis_index("rep")
    copies = []
    for at, (row, column) in enumerate(places):
        start = pl.multiple_of(column(me) * width, width)
        target = out_ref.at[pl.ds(row, pieces[at].shape[0]), pl.ds(start, width)]
        copies.append(pltpu.make_async_copy(pieces[at], target, sems.at[at]))
    for one in copies:
        one.start()
    for one in copies:
        one.wait()


def place(out, shape, entries):
    pieces = [e[0] for e in entries]
    kernel = functools.partial(place_kernel, [e[1:] for e in entries], pieces[0].shape[1])
    more = [] if out is None else [out]
    return pl.pallas_call(
        kernel,
        out_shape=jax.ShapeDtypeStruct(shape, pieces[0].dtype),
        in_specs=[ANY] * (len(pieces) + len(more)),
        out_specs=ANY,
        scratch_shapes=[pltpu.SemaphoreType.DMA((len(pieces),))],
        input_output_aliases={len(pieces): 0} if more else {},
        compiler_params=params(16),
    )(*pieces, *more)


def gather_columns(halves, rep):
    half, width = halves[0].shape
    shape = (2 * half, rep * width)
    chips = rep // 2
    hops = chips // 2

    def hop(piece, step):
        pairs = [(z * 2 + c, ((z + step) % chips) * 2 + c) for z in range(chips) for c in range(2)]
        return lax.ppermute(piece, "rep", pairs)

    def entries(piece, which, step):
        def column(other):
            def of(me):
                return lax.rem(me // 2 + chips - step, chips) * 2 + ((me & 1) ^ other)
            return of

        swapped = lax.ppermute(piece, "rep", [(r, r ^ 1) for r in range(rep)])
        return [(piece, which * half, column(0)), (swapped, which * half, column(1))]

    out, waiting, own = None, [], []
    moving = [[halves[0]], [halves[1]]]
    for step in range(hops + 1):
        for which in range(2):
            pieces = moving[which]
            if step == 0:
                moving[which] = [hop(pieces[0], 1), hop(pieces[0], -1)]
                own.append(pieces[0])
                continue
            if own:
                *pieces, own[0], own[1] = lax.optimization_barrier((*pieces, *own))
            if out is not None:
                *pieces, out = lax.optimization_barrier((*pieces, out))
            if step < hops:
                keep = (True, True) if step + 1 < hops else (which == 0, which == 1)
                moving[which] = [hop(p, d) for p, d, k in zip(pieces, (1, -1), keep) if k]
                froms = [step, chips - step]
            else:
                froms = [hops]
            if waiting:
                out = place(out, shape, waiting)
            waiting = []
            for at, piece in enumerate(own):
                waiting += entries(piece, at, 0)
            own = []
            for piece, distance in zip(pieces, froms):
                waiting += entries(piece, which, distance)
    return place(out, shape, waiting)


def per_device(n, rep, gradient, row_counts, owners, refresh_flags, stat_left, stat_right, root_left, root_right):
    capacity, width = gradient.shape
    tile = stat_left.shape[-1]
    part, each, many = tile // n, capacity // n, width // LANES
    struct = jax.ShapeDtypeStruct

    def in_hbm(x):
        return pltpu.with_memory_space_constraint(x, pltpu.HBM)

    states = [in_hbm(x) for x in (stat_left, stat_right, root_left, root_right)]
    table = jnp.concatenate([row_counts, owners.reshape(-1), refresh_flags.reshape(-1)])

    def rows_of(count, strip_count=many):
        return pltpu.VMEM((strip_count, count, LANES), f32)

    def exchange(x):
        return lax.all_to_all(x, "fsdp", 0, 0, tiled=True)

    sent = pl.pallas_call(
        functools.partial(spread_kernel, n),
        out_shape=struct((n, many * each * 3 // 2 + 8, LANES), jnp.int16),
        in_specs=[SMEM, ANY], out_specs=VMEM,
        scratch_shapes=[rows_of(n * PAD), rows_of(many * each, n), pltpu.SemaphoreType.DMA((many,))],
        compiler_params=params(),
    )(table, in_hbm(gradient))
    sent = pl.pallas_call(
        functools.partial(collect_kernel, n, width),
        out_shape=struct((n, many * part * 3 // 2 + 16, LANES), jnp.int16),
        in_specs=[SMEM, VMEM], out_specs=VMEM,
        scratch_shapes=[rows_of(many * each, n), rows_of(tile + PAD)],
        compiler_params=params(),
    )(table, exchange(sent))
    square = (tile, tile)
    new_left, new_right, tiles = pl.pallas_call(
        functools.partial(update_kernel, n),
        out_shape=(struct(stat_left.shape, f32), struct(stat_right.shape, f32))
        + (struct((n, part, width), bf16),),
        in_specs=[SMEM, VMEM, ANY, ANY, ANY, ANY],
        out_specs=(ANY, ANY, VMEM),
        scratch_shapes=[
            rows_of(tile), pltpu.VMEM((2,) + square, f32), pltpu.VMEM((2,) + square, f32),
            pltpu.VMEM((10,) + square, bf16), pltpu.VMEM((10,) + square, bf16),
            rows_of(tile), pltpu.SemaphoreType.DMA((6,)),
        ],
        compiler_params=params(36),
    )(table, exchange(sent), *states)

    sent = pl.pallas_call(
        functools.partial(scatter_kernel, n),
        out_shape=struct((n, many * each, LANES), bf16),
        in_specs=[SMEM, VMEM], out_specs=VMEM,
        scratch_shapes=[rows_of(tile + PAD), rows_of(many * each, n)],
        compiler_params=params(),
    )(table, exchange(tiles))
    half = struct((capacity // 2, width), bf16)
    halves = pl.pallas_call(
        functools.partial(merge_kernel, n),
        out_shape=(half, half),
        in_specs=[SMEM, VMEM], out_specs=(VMEM, VMEM),
        scratch_shapes=[rows_of(many * each, n), rows_of(n * PAD)],
        compiler_params=params(),
    )(table, exchange(sent))
    return gather_columns(halves, rep), new_left, new_right


def solution(mesh):
    state = P("fsdp", "rep", None, None)
    return jax.shard_map(
        functools.partial(per_device, mesh.shape["fsdp"], mesh.shape["rep"]),
        mesh=mesh,
        in_specs=(P("fsdp", "rep"), P(), P(None, "rep"), P(None, "rep"), state, state, state, state),
        out_specs=(P("fsdp", None), state, state),
        check_vma=False,
    )
```
